32 devices in a mesh: data: 8 (over z, y), width: 4 (over x, core).
Axes of the slice: x: 2, y: 2, z: 4, core: 2. Of those that a mesh axis runs over, the one named last changes fastest.
Arguments:
- grad_up: float32 [8, 768, 3072], P('data', None, 'width'), may hold values from -4 to 4
- grad_down: float32 [8, 3072, 768], P('data', 'width'), may hold values from -4 to 4
- grad_query: float32 [8, 768, 768], P('data', None, 'width'), may hold values from -4 to 4
- grad_key: float32 [8, 768, 768], P('data', None, 'width'), may hold values from -4 to 4
- grad_value: float32 [8, 768, 768], P('data', None, 'width'), may hold values from -4 to 4
- grad_mixed: float32 [8, 768, 768], P('data', 'width'), may hold values from -4 to 4
- grad_norm: float32 [8, 768], P('data'), may hold values from -8 to 8
- weight_up: float32 [768, 3072], P('data', 'width'), may hold values from -0.21875 to 0.21875
- weight_down: float32 [3072, 768], P('width', 'data'), may hold values from -0.109375 to 0.109375
- weight_query: float32 [768, 768], P('data', 'width'), may hold values from -0.21875 to 0.21875
- weight_key: float32 [768, 768], P('data', 'width'), may hold values from -0.21875 to 0.21875
- weight_value: float32 [768, 768], P('data', 'width'), may hold values from -0.21875 to 0.21875
- weight_mixed: float32 [768, 768], P('width', 'data'), may hold values from -0.21875 to 0.21875
- weight_norm: float32 [768], P('data'), may hold values from 0.25 to 1.75
- moment_up: float32 [768, 3072], P('data', 'width'), may hold values from 0.05 to 0.8
- moment_down: float32 [3072, 768], P('width', 'data'), may hold values from 0.05 to 0.8
- moment_query: float32 [768, 768], P('data', 'width'), may hold values from 0.05 to 0.8
- moment_key: float32 [768, 768], P('data', 'width'), may hold values from 0.05 to 0.8
- moment_value: float32 [768, 768], P('data', 'width'), may hold values from 0.05 to 0.8
- moment_mixed: float32 [768, 768], P('width', 'data'), may hold values from 0.05 to 0.8
- moment_norm: float32 [768], P('data'), may hold values from 0.05 to 0.8
Outputs:
- copy_up: bfloat16 [768, 3072], P(None, 'width')
- copy_down: bfloat16 [3072, 768], P('width')
- copy_query: bfloat16 [768, 768], P(None, 'width')
- copy_key: bfloat16 [768, 768], P(None, 'width')
- copy_value: bfloat16 [768, 768], P(None, 'width')
- copy_mixed: bfloat16 [768, 768], P('width')
- copy_norm: bfloat16 [768], replicated
- new_up: float32 [768, 3072], P('data', 'width')
- new_down: float32 [3072, 768], P('width', 'data')
- new_query: float32 [768, 768], P('data', 'width')
- new_key: float32 [768, 768], P('data', 'width')
- new_value: float32 [768, 768], P('data', 'width')
- new_mixed: float32 [768, 768], P('width', 'data')
- new_norm: float32 [768], P('data')
- state_new_up: float32 [768, 3072], P('data', 'width')
- state_new_down: float32 [3072, 768], P('width', 'data')
- state_new_query: float32 [768, 768], P('data', 'width')
- state_new_key: float32 [768, 768], P('data', 'width')
- state_new_value: float32 [768, 768], P('data', 'width')
- state_new_mixed: float32 [768, 768], P('width', 'data')
- state_new_norm: float32 [768], P('data')
The draws below stay inside these ranges and needn't reach their ends.
All inputs are finite; a program needn't handle non-finite values.
Results may differ from the reference program's by a relative error of at most 0.0004.
Values may be sent and summed in bfloat16 or wider, within the bound.
No kernel may reach another device: no remote copies, remote signals or barrier semaphores. Data moves between devices by JAX's collectives and lax.ppermute only.
A program may use at most 128 MiB of HBM per device.

```python
import jax
import jax.numpy as jnp
from jax import lax

WIDTH = 768
INNER = 3072
ATTN = 768
REPLICAS = 8


def raised(entries, stream_key, source, target, parts, factor):
    owner, partner = [(jnp.arange(entries.shape[axis_at]) // (entries.shape[axis_at] // parts)).reshape([-1 if axis == axis_at else 1 for axis in range(entries.ndim)]) for axis_at in (source, target)]
    chosen = jax.random.permutation(stream_key, parts)[partner]
    strong = (owner == chosen) | (owner == (partner + parts // 2) % parts)
    return jnp.where(strong, factor * entries, entries)


def block_scale(key, dims, split, smallest, largest):
    def one(dim, shards_of):
        draws = jax.random.uniform(jax.random.fold_in(jax.random.fold_in(key, 6), dim), (shards_of,), jnp.float32, smallest / len(split), largest / len(split))
        return jnp.repeat(jnp.exp(draws), dims[dim] // shards_of).reshape((-1,) + (1,) * (len(dims) - dim - 1))

    loudness = one(*split[0])
    for cut in split[1:]:
        loudness = loudness * one(*cut)
    return loudness


def scatter_about(own_key, extent, deviation, reach, split=(), held_as=jnp.bfloat16):
    factor_of = block_scale(own_key, extent, split, -0.22, 0.18) if split else 1.0
    drawn = jax.random.normal(own_key, extent, jnp.float32) * deviation * factor_of
    return jnp.minimum(jnp.maximum(drawn, -reach), reach).astype(held_as)


def noise_with(rng, dims, width, reach, pieces, heavy, kind=jnp.bfloat16):
    drawn = width * jax.random.normal(rng, dims, jnp.float32)
    if pieces:
        drawn = drawn * block_scale(rng, dims, pieces, -0.22, 0.18)
    return jnp.clip(raised(drawn, jax.random.fold_in(rng, 3), *heavy), -reach, reach).astype(kind)


def setup_inputs(seed: int = 0) -> dict:
    keys = jax.random.split(jax.random.key(seed), 22)
    grad_up = noise_with(keys[0], (REPLICAS, WIDTH, INNER), 0.5, 4.0, ((0, 8), (2, 4)), (0, 1, 8, 2.0), jnp.float32)
    grad_down = noise_with(keys[1], (REPLICAS, INNER, WIDTH), 0.5, 4.0, ((0, 8), (1, 4)), (0, 2, 8, 2.0), jnp.float32)
    grad_query = noise_with(keys[2], (REPLICAS, WIDTH, ATTN), 0.5, 4.0, ((0, 8), (2, 4)), (0, 1, 8, 2.0), jnp.float32)
    grad_key = noise_with(keys[3], (REPLICAS, WIDTH, ATTN), 0.5, 4.0, ((0, 8), (2, 4)), (0, 1, 8, 2.0), jnp.float32)
    grad_value = noise_with(keys[4], (REPLICAS, WIDTH, ATTN), 0.5, 4.0, ((0, 8), (2, 4)), (0, 1, 8, 2.0), jnp.float32)
    grad_mixed = noise_with(keys[5], (REPLICAS, ATTN, WIDTH), 0.5, 4.0, ((0, 8), (1, 4)), (0, 2, 8, 2.0), jnp.float32)
    grad_norm = noise_with(keys[6], (REPLICAS, WIDTH), 1.0, 8.0, ((0, 8),), (0, 1, 8, 2.0), jnp.float32)
    weight_up = scatter_about(keys[7], (WIDTH, INNER), WIDTH ** -0.5, 0.21875, ((0, 8), (1, 4)), jnp.float32)
    weight_down = scatter_about(keys[8], (INNER, WIDTH), INNER ** -0.5, 0.109375, ((0, 4), (1, 8)), jnp.float32)
    weight_query = scatter_about(keys[9], (WIDTH, ATTN), WIDTH ** -0.5, 0.21875, ((0, 8), (1, 4)), jnp.float32)
    weight_key = scatter_about(keys[10], (WIDTH, ATTN), WIDTH ** -0.5, 0.21875, ((0, 8), (1, 4)), jnp.float32)
    weight_value = scatter_about(keys[11], (WIDTH, ATTN), WIDTH ** -0.5, 0.21875, ((0, 8), (1, 4)), jnp.float32)
    weight_mixed = scatter_about(keys[12], (ATTN, WIDTH), ATTN ** -0.5, 0.21875, ((0, 4), (1, 8)), jnp.float32)
    weight_norm = jnp.clip(1.0 + 0.15 * jax.random.normal(keys[13], (WIDTH,), jnp.float32), 0.25, 1.75)
    moment_up = jnp.clip(0.05 + 0.75 * jax.random.uniform(keys[14], (WIDTH, INNER), jnp.float32) ** block_scale(keys[14], (WIDTH, INNER), ((0, 8), (1, 4)), -0.2, 0.2), 0.05, 0.8)
    moment_down = jnp.clip(0.05 + 0.75 * jax.random.uniform(keys[15], (INNER, WIDTH), jnp.float32) ** block_scale(keys[15], (INNER, WIDTH), ((0, 4), (1, 8)), -0.2, 0.2), 0.05, 0.8)
    moment_query = jnp.clip(0.05 + 0.75 * jax.random.uniform(keys[16], (WIDTH, ATTN), jnp.float32) ** block_scale(keys[16], (WIDTH, ATTN), ((0, 8), (1, 4)), -0.2, 0.2), 0.05, 0.8)
    moment_key = jnp.clip(0.05 + 0.75 * jax.random.uniform(keys[17], (WIDTH, ATTN), jnp.float32) ** block_scale(keys[17], (WIDTH, ATTN), ((0, 8), (1, 4)), -0.2, 0.2), 0.05, 0.8)
    moment_value = jnp.clip(0.05 + 0.75 * jax.random.uniform(keys[18], (WIDTH, ATTN), jnp.float32) ** block_scale(keys[18], (WIDTH, ATTN), ((0, 8), (1, 4)), -0.2, 0.2), 0.05, 0.8)
    moment_mixed = jnp.clip(0.05 + 0.75 * jax.random.uniform(keys[19], (ATTN, WIDTH), jnp.float32) ** block_scale(keys[19], (ATTN, WIDTH), ((0, 4), (1, 8)), -0.2, 0.2), 0.05, 0.8)
    moment_norm = jnp.clip(0.05 + 0.75 * jax.random.uniform(keys[20], (WIDTH,), jnp.float32) ** block_scale(keys[20], (WIDTH,), ((0, 8),), -0.2, 0.2), 0.05, 0.8)
    return dict(grad_up=grad_up, grad_down=grad_down, grad_query=grad_query, grad_key=grad_key, grad_value=grad_value, grad_mixed=grad_mixed, grad_norm=grad_norm, weight_up=weight_up, weight_down=weight_down, weight_query=weight_query, weight_key=weight_key, weight_value=weight_value, weight_mixed=weight_mixed, weight_norm=weight_norm, moment_up=moment_up, moment_down=moment_down, moment_query=moment_query, moment_key=moment_key, moment_value=moment_value, moment_mixed=moment_mixed, moment_norm=moment_norm)


learn_rate = 0.05
hold_rate = 0.9

def reference(grad_up, grad_down, grad_query, grad_key, grad_value, grad_mixed, grad_norm, weight_up, weight_down, weight_query, weight_key, weight_value, weight_mixed, weight_norm, moment_up, moment_down, moment_query, moment_key, moment_value, moment_mixed, moment_norm):
    mean_up = lax.optimization_barrier(jnp.sum(grad_up.astype(jnp.float32), axis=0)) * REPLICAS ** (-0.5)
    mean_down = lax.optimization_barrier(jnp.sum(grad_down.astype(jnp.float32), axis=0)) * REPLICAS ** (-0.5)
    mean_query = lax.optimization_barrier(jnp.sum(grad_query.astype(jnp.float32), axis=0)) * REPLICAS ** (-0.5)
    mean_key = lax.optimization_barrier(jnp.sum(grad_key.astype(jnp.float32), axis=0)) * REPLICAS ** (-0.5)
    mean_value = lax.optimization_barrier(jnp.sum(grad_value.astype(jnp.float32), axis=0)) * REPLICAS ** (-0.5)
    mean_mixed = lax.optimization_barrier(jnp.sum(grad_mixed.astype(jnp.float32), axis=0)) * REPLICAS ** (-0.5)
    mean_norm = lax.optimization_barrier(jnp.sum(grad_norm.astype(jnp.float32), axis=0)) * REPLICAS ** (-0.5)
    state_new_up = hold_rate * moment_up + (1.0 - hold_rate) * mean_up * mean_up
    new_up = weight_up - learn_rate * mean_up * lax.rsqrt(state_new_up + 1e-06)
    state_new_down = hold_rate * moment_down + (1.0 - hold_rate) * mean_down * mean_down
    new_down = weight_down - learn_rate * mean_down * lax.rsqrt(state_new_down + 1e-06)
    state_new_query = hold_rate * moment_query + (1.0 - hold_rate) * mean_query * mean_query
    new_query = weight_query - learn_rate * mean_query * lax.rsqrt(state_new_query + 1e-06)
    state_new_key = hold_rate * moment_key + (1.0 - hold_rate) * mean_key * mean_key
    new_key = weight_key - learn_rate * mean_key * lax.rsqrt(state_new_key + 1e-06)
    state_new_value = hold_rate * moment_value + (1.0 - hold_rate) * mean_value * mean_value
    new_value = weight_value - learn_rate * mean_value * lax.rsqrt(state_new_value + 1e-06)
    state_new_mixed = hold_rate * moment_mixed + (1.0 - hold_rate) * mean_mixed * mean_mixed
    new_mixed = weight_mixed - learn_rate * mean_mixed * lax.rsqrt(state_new_mixed + 1e-06)
    state_new_norm = hold_rate * moment_norm + (1.0 - hold_rate) * mean_norm * mean_norm
    new_norm = weight_norm - learn_rate * mean_norm * lax.rsqrt(state_new_norm + 1e-06)
    copy_up = new_up.astype(jnp.bfloat16)
    copy_down = new_down.astype(jnp.bfloat16)
    copy_query = new_query.astype(jnp.bfloat16)
    copy_key = new_key.astype(jnp.bfloat16)
    copy_value = new_value.astype(jnp.bfloat16)
    copy_mixed = new_mixed.astype(jnp.bfloat16)
    copy_norm = new_norm.astype(jnp.bfloat16)
    return (copy_up, copy_down, copy_query, copy_key, copy_value, copy_mixed, copy_norm, new_up, new_down, new_query, new_key, new_value, new_mixed, new_norm, state_new_up, state_new_down, state_new_query, state_new_key, state_new_value, state_new_mixed, state_new_norm)
```

```python
import jax
import jax.numpy as jnp
from jax import lax
from jax.sharding import PartitionSpec as P
from jax.experimental import pallas as pl
from jax.experimental.pallas import tpu as pltpu

learn_rate = 0.05
hold_rate = 0.9


class Plan:
    def __init__(self):
        self.count = lax.axis_size("data")
        self.wide = lax.axis_size("width")
        self.levels = self.count.bit_length() - 1
        even = list(range(self.levels))
        odd = even[1::-1] + even[2:]
        self.orders = (even, odd)
        self.place = lax.axis_index("data")
        self.odd = (lax.axis_index("width") & 1) == 1

    def pairs(self, step):
        flips = [1 << o[step] for o in self.orders]
        return [
            (d * self.wide + w, (d ^ flips[w & 1]) * self.wide + w)
            for d in range(self.count) for w in range(self.wide)
        ]

    def swap(self, block, step):
        return lax.ppermute(block, ("data", "width"), self.pairs(step))

    def chunk_of(self, slot):
        one = [sum(((slot >> (self.levels - 1 - i)) & 1) << o[i] for i in range(self.levels)) for o in self.orders]
        return self.place ^ jnp.where(self.odd, one[1], one[0])

    def slot_of(self, chunk):
        x = self.place ^ chunk
        one = [sum(((x >> o[i]) & 1) << (self.levels - 1 - i) for i in range(self.levels)) for o in self.orders]
        return jnp.where(self.odd, one[1], one[0])


def pick(block, ids):
    return jnp.concatenate([lax.dynamic_slice_in_dim(block, i, 1, 0) for i in ids], 0)


def scatter_sum(plan, block):
    n = plan.count
    block = block.reshape(n, block.shape[0] // n, block.shape[1])
    half = n // 2
    sent = pick(block, [plan.chunk_of(half + j) for j in range(half)])
    got = plan.swap(sent, 0)
    kept = pick(block, [plan.chunk_of(j) for j in range(half)])
    terms = [kept, got]
    for step in range(1, plan.levels):
        half //= 2
        sent = terms[0][half:2 * half]
        for t in terms[1:]:
            sent = sent + t[half:2 * half]
        terms.append(plan.swap(sent, step))
    total = terms[0][0]
    for t in terms[1:]:
        total = total + t[0]
    return total


def gather(plan, block):
    block = block[None]
    for step in reversed(range(plan.levels)):
        block = jnp.concatenate([block, plan.swap(block, step)], 0)
    out = pick(block, [plan.slot_of(d) for d in range(plan.count)])
    return out.reshape(-1, out.shape[-1])


def update(total, weight, moment, rate):
    mean = total * rate
    state = hold_rate * moment + (1.0 - hold_rate) * mean * mean
    return weight - learn_rate * mean * lax.rsqrt(state + 1e-06), state


def on_device(*args):
    g_up, g_down, g_query, g_key, g_value, g_mixed, g_norm = (a[0] for a in args[:7])
    w_up, w_down, w_query, w_key, w_value, w_mixed, w_norm = args[7:14]
    m_up, m_down, m_query, m_key, m_value, m_mixed, m_norm = args[14:]
    plan = Plan()
    count = plan.count
    rate = count ** (-0.5)
    rows = g_up.shape[0] // count
    thin = g_query.shape[1]
    bf = jnp.bfloat16

    at = plan.place
    slot = lambda v: lax.dynamic_update_slice(jnp.zeros((count * rows,), v.dtype), v, (at * rows,))
    norm = jnp.stack([g_norm, slot(w_norm), slot(m_norm)])
    for step in range(plan.levels):
        norm = norm + plan.swap(norm, step)
    n_norm, s_norm = update(norm[0], norm[1], norm[2], rate)
    c_norm = n_norm.astype(bf)
    n_norm, s_norm = (lax.dynamic_slice(v, (at * rows,), (rows,)) for v in (n_norm, s_norm))

    g_d = lax.optimization_barrier(g_down.T)
    g_c = lax.optimization_barrier(jnp.concatenate([g_query, g_key, g_value, g_mixed.T], 1))
    t_u = scatter_sum(plan, g_up)
    t_d = scatter_sum(plan, g_d)
    t_c = scatter_sum(plan, g_c)
    n_u, s_u = update(t_u, w_up, m_up, rate)
    n_d, s_d = update(t_d, w_down.T, m_down.T, rate)
    w_c = jnp.concatenate([w_query, w_key, w_value, w_mixed.T], 1)
    m_c = jnp.concatenate([m_query, m_key, m_value, m_mixed.T], 1)
    n_c, s_c = update(t_c, w_c, m_c, rate)
    c_u = gather(plan, n_u.astype(bf))
    c_d = gather(plan, n_d.astype(bf))
    c_c = gather(plan, n_c.astype(bf))
    four = lambda v: [v[:, i * thin:(i + 1) * thin] for i in range(3)] + [v[:, 3 * thin:].T]
    return (
        c_u, c_d.T, *four(c_c), c_norm,
        n_u, n_d.T, *four(n_c), n_norm,
        s_u, s_d.T, *four(s_c), s_norm,
    )


def solution(mesh):
    return jax.shard_map(
        on_device,
        mesh=mesh,
        in_specs=(
            P("data", None, "width"),
            P("data", "width", None),
            P("data", None, "width"),
            P("data", None, "width"),
            P("data", None, "width"),
            P("data", "width", None),
            P("data", None),
            P("data", "width"),
            P("width", "data"),
            P("data", "width"),
            P("data", "width"),
            P("data", "width"),
            P("width", "data"),
            P("data"),
            P("data", "width"),
            P("width", "data"),
            P("data", "width"),
            P("data", "width"),
            P("data", "width"),
            P("width", "data"),
            P("data"),
        ),
        out_specs=(
            P(None, "width"),
            P("width", None),
            P(None, "width"),
            P(None, "width"),
            P(None, "width"),
            P("width", None),
            P(),
            P("data", "width"),
            P("width", "data"),
            P("data", "width"),
            P("data", "width"),
            P("data", "width"),
            P("width", "data"),
            P("data"),
            P("data", "width"),
            P("width", "data"),
            P("data", "width"),
            P("data", "width"),
            P("data", "width"),
            P("width", "data"),
            P("data"),
        ),
        check_vma=False,
    )
```
